32 devices in a mesh: gx: 2 (over x), gy: 4 (over y, core), gz: 4 (over z).
Axes of the slice: x: 2, y: 2, z: 4, core: 2. Of those that a mesh axis runs over, the one named last changes fastest.
Arguments:
- metric_pert: float32 [6, 32, 64, 512], P(None, 'gx', 'gy', 'gz'), may hold values from -1.8 to 1.8
- curvature: float32 [6, 32, 64, 512], P(None, 'gx', 'gy', 'gz'), may hold values from -6 to 6
- interp_weights: bfloat16 [2, 4, 32, 64, 4096], P('gx', 'gy', 'gz'), may hold values from -0.09375 to 0.09375
- point_ids: int32 [2, 4, 32, 64], P('gx', 'gy', 'gz'), may hold values from 0 to 6144, as said below
- theta: float32 [6144], replicated, may hold values from 0.05 to 3.09
- phi: float32 [6144], replicated, may hold values from -3.140625 to 3.140625
Outputs:
- psi4_field: bfloat16 [2, 32, 64, 512], P(None, 'gx', 'gy', 'gz')
- modes: float32 [3, 2, 77], replicated
The draws below stay inside these ranges and needn't reach their ends.
Inputs may be any that keep to these rules, and one draw needn't show every extreme that they name: `point_ids`: the grid is a window of the extraction region that the spheres cross. A live entry names a sphere point; the value 6144 marks an empty slot, and each list holds its live entries first. The points of sphere s lie in the 9 consecutive block layers along the third dimension that begin at layer s * 10; each point belongs to one column (bx, by) and is listed in exactly two blocks of that column that are adjacent along the third dimension. Some block's list is full, every listing block holds at least 32 live entries, and blocks outside these layers list no point.
All inputs are finite; a program needn't handle non-finite values.
Results may differ from the reference program's by a relative error of at most 0.0032.
Values sent between devices are 32-bit elements; how exact they have to be, the bound alone decides.
A program may use at most 64 MiB of HBM per device.

```python
import math
import jax
import jax.numpy as jnp
import numpy as np
from jax import lax

BLK = 16
PB = 64
PTS = 2048
SPHERES = 3
LMAX = 8
NX = 32
NY = 64
NZ = 512
NBX = 2
NBY = 4
NBZ = 32
COL_PTS = 256
RUNS = 8
TOTAL_PTS = 6144


def draw_point_ids(key, part):
    columns = NBX * NBY
    half = PB // 2
    keys = jax.random.split(key, SPHERES * columns)
    orders = jax.vmap(lambda subkey: jax.random.permutation(subkey, COL_PTS))(keys).reshape(SPHERES, columns, COL_PTS)
    base = (jnp.arange(SPHERES) * PTS)[:, None, None] + (jnp.arange(columns) * COL_PTS)[None, :, None]
    listed = (base + orders).astype(jnp.int32).reshape(SPHERES, columns, RUNS, half)
    layer = jnp.arange(RUNS + 1)
    earlier = listed[:, :, jnp.maximum(layer - 1, 0)]
    current = listed[:, :, jnp.minimum(layer, RUNS - 1)]
    live = ((layer >= 1) & (layer <= RUNS - 1))[None, None, :, None]
    current = jnp.where(live, current, TOTAL_PTS)
    lists = jnp.concatenate([earlier, current], 3).astype(jnp.int32)
    result = jnp.full((columns, NBZ, PB), TOTAL_PTS, jnp.int32)
    spacing = NBZ // SPHERES
    for sphere in range(SPHERES):
        result = result.at[:, sphere * spacing:sphere * spacing + RUNS + 1].set(lists[sphere])
    return result.reshape(NBX, NBY, NBZ, PB).astype(jnp.int32)


def levels(stream_key, shape, pieces, low, high):
    factor_of, own = 1.0, jax.random.fold_in(stream_key, 6)
    for dim, shards_of in pieces:
        heights = jnp.exp(jax.random.uniform(jax.random.fold_in(own, dim), (shards_of,), jnp.float32, low / len(pieces), high / len(pieces)))
        factor_of = factor_of * jnp.repeat(heights, shape[dim] // shards_of).reshape([-1 if axis == dim else 1 for axis in range(len(shape))])
    return factor_of


def normal_values(own_key, shape, scale, reach, pieces=(), held_as=jnp.bfloat16):
    values = scale * jax.random.normal(own_key, shape, jnp.float32)
    if pieces:
        values = values * levels(own_key, shape, pieces, -0.22, 0.18)
    return jnp.clip(values, -reach, reach).astype(held_as)


def setup_inputs(seed: int = 0) -> dict:
    key_list = jax.random.split(jax.random.key(seed), 7)
    return {
        "metric_pert": normal_values(key_list[0], (6, NX, NY, NZ), 0.3, 1.8, ((1, 2), (2, 4), (3, 4)), jnp.float32),
        "curvature": normal_values(key_list[1], (6, NX, NY, NZ), 1.0, 6.0, ((1, 2), (2, 4), (3, 4)), jnp.float32),
        "interp_weights": normal_values(key_list[2], (NBX, NBY, NBZ, PB, BLK * BLK * BLK), (BLK * BLK * BLK) ** -0.5, 0.09375, ((0, 2), (1, 4), (2, 4))),
        "point_ids": draw_point_ids(jax.random.fold_in(key_list[6], 71), 0),
        "theta": jnp.clip(jax.random.uniform(key_list[4], (TOTAL_PTS,), jnp.float32, 0.05, 3.09), 0.05, 3.09),
        "phi": jnp.clip(jax.random.uniform(key_list[5], (TOTAL_PTS,), jnp.float32, -3.140625, 3.140625), -3.140625, 3.140625),
    }


PAIRS = [[0, 1, 2], [1, 3, 4], [2, 4, 5]]

def build_table(degree_max):
    width = 2 * degree_max + 1
    columns = []
    orders = []
    for degree in range(2, degree_max + 1):
        for order in range(-degree, degree + 1):
            column = np.zeros(width * width)
            lead = (-1.0) ** order * math.sqrt(math.factorial(degree + order) * math.factorial(degree - order) * (2 * degree + 1) / (4.0 * math.pi * math.factorial(degree - 2) * math.factorial(degree + 2)))
            for step in range(0, degree + 3):
                lower = step - 2 - order
                if lower >= 0 and lower <= degree - 2:
                    value = lead * math.comb(degree + 2, step) * math.comb(degree - 2, lower) * (-1.0) ** (degree - step + 2)
                    expo = 2 * step - 2 - order
                    column[expo * width + (2 * degree - expo)] += value
            columns.append(column)
            orders.append(order)
    return (np.stack(columns, 1), np.array(orders))

def project(sphere_vals, theta, phi, member):
    table, orders = build_table(LMAX)
    width = 2 * LMAX + 1
    cosine = jnp.cos(theta * 0.5)
    sine = jnp.sin(theta * 0.5)
    cos_pow = jnp.stack([cosine ** power for power in range(width)], 1)
    sin_pow = jnp.stack([sine ** power for power in range(width)], 1)
    grid_pow = (cos_pow[:, :, None] * sin_pow[:, None, :]).reshape(theta.shape[0], width * width)
    amplitude = jnp.dot(grid_pow, jnp.asarray(table, jnp.float32), precision=lax.Precision.HIGHEST)
    angle_m = phi[:, None] * jnp.asarray(orders, jnp.float32)[None, :]
    y_real = amplitude * jnp.cos(angle_m)
    y_imag = amplitude * jnp.sin(angle_m)
    left_re = member * sphere_vals[0][None, :]
    left_im = member * sphere_vals[1][None, :]
    highest = lax.Precision.HIGHEST
    real = jnp.dot(left_re, y_real, precision=highest) + jnp.dot(left_im, y_imag, precision=highest)
    imag = jnp.dot(left_im, y_real, precision=highest) - jnp.dot(left_re, y_imag, precision=highest)
    return jnp.stack([real, imag], 1) * (4.0 * math.pi / PTS)

def weyl_scalar(padded, x_coord, y_coord, z_coord):
    extent = [x_coord.shape[0], y_coord.shape[0], z_coord.shape[0]]

    def moved(comp, axis, offset):
        index = [slice(2, 2 + count) for count in extent]
        index[axis] = slice(2 + offset, 2 + offset + extent[axis])
        return padded[comp][tuple(index)]

    def first(comp, axis):
        return (moved(comp, axis, -2) - 8.0 * moved(comp, axis, -1) + 8.0 * moved(comp, axis, 1) - moved(comp, axis, 2)) / 12.0

    def second(comp, axis):
        return (-moved(comp, axis, -2) + 16.0 * moved(comp, axis, -1) - 30.0 * moved(comp, axis, 0) + 16.0 * moved(comp, axis, 1) - moved(comp, axis, 2)) / 12.0
    kval = [moved(6 + comp, 0, 0) for comp in range(6)]
    trace = kval[0] + kval[3] + kval[5]
    electric = {}
    for row in range(3):
        for col in range(row, 3):
            comp = PAIRS[row][col]
            laplace = second(comp, 0) + second(comp, 1) + second(comp, 2)
            square = kval[PAIRS[row][0]] * kval[PAIRS[0][col]] + kval[PAIRS[row][1]] * kval[PAIRS[1][col]] + kval[PAIRS[row][2]] * kval[PAIRS[2][col]]
            value = -0.5 * laplace + trace * kval[comp] - square
            electric[row, col] = value
            electric[col, row] = value
    deriv = [[first(6 + comp, axis) for comp in range(6)] for axis in range(3)]
    curl = {}
    for row in range(3):
        one = (row + 1) % 3
        two = (row + 2) % 3
        for col in range(3):
            curl[row, col] = deriv[one][PAIRS[two][col]] - deriv[two][PAIRS[one][col]]
    x_full = x_coord[:, None, None]
    y_full = y_coord[None, :, None]
    z_full = z_coord[None, None, :]
    radial_xy = jnp.sqrt(x_full * x_full + y_full * y_full)
    radius = jnp.sqrt(radial_xy * radial_xy + z_full * z_full)
    cos_phi = x_full / radial_xy
    sin_phi = y_full / radial_xy
    cos_theta = z_full / radius
    sin_theta = radial_xy / radius
    e_theta = [cos_theta * cos_phi, cos_theta * sin_phi, -sin_theta]
    e_phi = [-sin_phi, cos_phi, 0.0 * cos_phi]
    real = 0.0
    imag = 0.0
    for row in range(3):
        for col in range(3):
            magnetic = 0.5 * (curl[row, col] + curl[col, row])
            plus = 0.5 * (e_theta[row] * e_theta[col] - e_phi[row] * e_phi[col])
            cross = 0.5 * (e_theta[row] * e_phi[col] + e_phi[row] * e_theta[col])
            real = real + electric[row, col] * plus - magnetic * cross
            imag = imag - electric[row, col] * cross - magnetic * plus
    return jnp.stack([real, imag]).astype(jnp.float32)

def reference(metric_pert, curvature, interp_weights, point_ids, theta, phi):
    fields = jnp.concatenate([metric_pert, curvature], 0)
    padded = jnp.pad(fields, ((0, 0), (2, 2), (2, 2), (2, 2)))
    size_x, size_y, size_z = (metric_pert.shape[1], metric_pert.shape[2], metric_pert.shape[3])
    y_coord = jnp.arange(size_y).astype(jnp.float32) + 0.5 - size_y / 2.0
    z_coord = jnp.arange(size_z).astype(jnp.float32) + 0.5 - size_z / 2.0
    slabs = []
    dense = jnp.zeros((TOTAL_PTS + 1, 2), jnp.float32)
    for block_x in range(NBX):
        slab = padded[:, block_x * BLK:block_x * BLK + BLK + 4]
        x_coord = (jnp.arange(BLK) + block_x * BLK).astype(jnp.float32) + 0.5 - size_x / 2.0
        psi_slab = weyl_scalar(slab, x_coord, y_coord, z_coord).astype(jnp.bfloat16)
        slabs.append(psi_slab)
        blocks = psi_slab.reshape(2, BLK, NBY, BLK, NBZ, BLK).transpose(2, 4, 0, 1, 3, 5).reshape(NBY, NBZ, 2, BLK * BLK * BLK)
        partial_value = jnp.einsum('yzcn,yzpn->yzpc', blocks.astype(jnp.float32), interp_weights[block_x].astype(jnp.float32), precision=lax.Precision.HIGHEST)
        dense = dense + jax.ops.segment_sum(partial_value.reshape(-1, 2), point_ids[block_x].reshape(-1), num_segments=TOTAL_PTS + 1)
    psi4_field = jnp.concatenate(slabs, 1)
    sphere_vals = dense[:TOTAL_PTS].T
    point_index = jnp.arange(TOTAL_PTS)
    member = (point_index[None, :] // PTS == jnp.arange(SPHERES)[:, None]).astype(jnp.float32)
    modes = project(sphere_vals, theta, phi, member)
    return (psi4_field, modes)
```

```python
import functools
import math

import jax
import jax.numpy as jnp
import numpy as np
from jax import lax
from jax.experimental import pallas as pl
from jax.experimental.pallas import tpu as pltpu
from jax.sharding import PartitionSpec as P

BLK = 16
PB = 64
PTS = 2048
SPHERES = 3
LMAX = 8
MODES = (LMAX + 1) ** 2 - 4
ROWS = -(-MODES // 8) * 8
AXES = ("gx", "gy", "gz")
PAIRS = [[0, 1, 2], [1, 3, 4], [2, 4, 5]]
MESH = pl.DeviceIdType.MESH
LO = 8


def build_table():
    table = np.zeros((ROWS, ROWS))
    for degree in range(2, LMAX + 1):
        base = degree * degree - 4
        for order in range(-degree, degree + 1):
            lead = (-1.0) ** order * math.sqrt(
                math.factorial(degree + order)
                * math.factorial(degree - order)
                * (2 * degree + 1)
                / (4.0 * math.pi * math.factorial(degree - 2) * math.factorial(degree + 2))
            )
            for step in range(0, degree + 3):
                lower = step - 2 - order
                if 0 <= lower <= degree - 2:
                    table[base + order + degree, base + 2 * step - 2 - order] += (
                        lead
                        * math.comb(degree + 2, step)
                        * math.comb(degree - 2, lower)
                        * (-1.0) ** (degree - step + 2)
                    )
    return table.astype(np.float32)


def power(bits, base, count):
    result = None
    for bit in range(count):
        factor = jnp.where((bits >> bit) & 1 == 1, base, 1.0)
        result = factor if result is None else result * factor
        base = base * base
    return result


def harmonics(ids, theta_ref, phi_ref, table):
    blocks, slots = ids.shape
    copies = 128 // slots
    wide = jnp.concatenate([ids] * copies, 1)
    safe = jnp.minimum(wide, SPHERES * PTS - 1)
    row, lane = safe >> 7, safe & 127
    theta = jnp.zeros(wide.shape, jnp.float32)
    phi = jnp.zeros(wide.shape, jnp.float32)
    for index in range(theta_ref.shape[0]):
        here = row == index
        one = jnp.broadcast_to(theta_ref[index : index + 1, :], wide.shape)
        theta = jnp.where(here, jnp.take_along_axis(one, lane, axis=1), theta)
        one = jnp.broadcast_to(phi_ref[index : index + 1, :], wide.shape)
        phi = jnp.where(here, jnp.take_along_axis(one, lane, axis=1), phi)

    def flat(array):
        return jnp.concatenate([array[b : b + 1, :slots] for b in range(blocks)], 1)

    half = theta * 0.5
    cosine, sine = flat(jnp.cos(half)), flat(jnp.sin(half))
    re, im = flat(jnp.cos(phi)), flat(jnp.sin(phi))
    sphere = flat(wide // PTS)
    k = lax.broadcasted_iota(jnp.int32, (ROWS, 1), 0)
    degree = jnp.full((ROWS, 1), 2, jnp.int32)
    for below in range(2, LMAX + 1):
        degree = degree + (k >= (below + 1) ** 2 - 4).astype(jnp.int32)
    first = k - (degree * degree - 4)
    order = first - degree
    mono = power(first, cosine, 5) * power(2 * degree - first, sine, 5)
    amplitude = jnp.dot(table, mono, precision=lax.Precision.HIGHEST, preferred_element_type=jnp.float32)
    size = jnp.abs(order)
    total_re = jnp.ones((ROWS, blocks * slots), jnp.float32)
    total_im = jnp.zeros((ROWS, blocks * slots), jnp.float32)
    for bit in range(4):
        on = (size >> bit) & 1 == 1
        f_re, f_im = jnp.where(on, re, 1.0), jnp.where(on, im, 0.0)
        total_re, total_im = total_re * f_re - total_im * f_im, total_re * f_im + total_im * f_re
        re, im = re * re - im * im, 2.0 * re * im
    total_im = jnp.where(order < 0, -total_im, total_im)
    return amplitude * total_re, amplitude * total_im, sphere


def weyl_tile(field, z_left, z_right, x, y, z):
    lane = lax.broadcasted_iota(jnp.int32, z.shape, 1)
    last = z.shape[1]

    def along(comp, axis, offset):
        if axis == 0:
            return field(comp, offset, 0)
        if axis == 1:
            return field(comp, 0, offset)
        edge = z_right if offset > 0 else z_left
        outside = lane < offset if offset > 0 else lane >= last + offset
        return pltpu.roll(jnp.where(outside, edge(comp), field(comp, 0, 0)), (-offset) % last, 1)

    def first(comp, axis):
        near = along(comp, axis, 1) - along(comp, axis, -1)
        far = along(comp, axis, 2) - along(comp, axis, -2)
        return near * (8.0 / 12.0) - far * (1.0 / 12.0)

    k = [field(6 + comp, 0, 0) for comp in range(6)]
    trace = k[0] + k[3] + k[5]
    electric = {}
    for row in range(3):
        for col in range(row, 3):
            comp = PAIRS[row][col]
            near, far = 0.0, 0.0
            for axis in range(3):
                near = near + (along(comp, axis, 1) + along(comp, axis, -1))
                far = far + (along(comp, axis, 2) + along(comp, axis, -2))
            laplace = near * (16.0 / 12.0) - far * (1.0 / 12.0) - field(comp, 0, 0) * 7.5
            square = sum(k[PAIRS[row][l]] * k[PAIRS[l][col]] for l in range(3))
            electric[row, col] = trace * k[comp] - square - 0.5 * laplace
    deriv = functools.lru_cache(None)(lambda axis, comp: first(6 + comp, axis))

    def curl(row, col):
        one, two = (row + 1) % 3, (row + 2) % 3
        return deriv(one, PAIRS[two][col]) - deriv(two, PAIRS[one][col])

    magnetic = {}
    for row in range(3):
        magnetic[row, row] = curl(row, row)
        for col in range(row + 1, 3):
            magnetic[row, col] = 0.5 * (curl(row, col) + curl(col, row))
    rho2 = x * x + y * y
    rho = jnp.sqrt(rho2)
    radius = jnp.sqrt(rho2 + z * z)
    inv_rho, inv_radius = 1.0 / rho, 1.0 / radius
    cos_phi, sin_phi = x * inv_rho, y * inv_rho
    cos_theta, sin_theta = z * inv_radius, rho * inv_radius
    t = [cos_theta * cos_phi, cos_theta * sin_phi, -sin_theta]
    p = [-sin_phi, cos_phi, None]
    real, imag = 0.0, 0.0
    for row in range(3):
        for col in range(row, 3):
            weight = 0.5 if row == col else 1.0
            plus = t[row] * t[col]
            if col < 2:
                plus = plus - p[row] * p[col]
            plus = plus * weight
            cross = None
            if row < 2:
                cross = p[row] * t[col]
                if col < 2:
                    cross = cross + t[row] * p[col]
                cross = cross * weight
            e, b = electric[row, col], magnetic[row, col]
            real = real + e * plus
            imag = imag - b * plus
            if cross is not None:
                real = real - b * cross
                imag = imag - e * cross
    return real, imag


def swap_blocks(tile):
    count = tile.shape[0]
    width = tile.shape[1] // count
    rolled = pltpu.roll(tile, 0, 1, stride=width, stride_axis=0)
    row = lax.broadcasted_iota(jnp.int32, tile.shape, 0)
    block = lax.broadcasted_iota(jnp.int32, tile.shape, 1) // width
    mixed = jnp.take_along_axis(rolled, (block - row + count) % count, axis=0)
    out = mixed
    for bit in range(3):
        shift = (1 << bit) * width
        out = jnp.where((row >> bit) & 1 == 1, pltpu.roll(out, tile.shape[1] - shift, 1), out)
    return out


def kernel(
    counts, metric, curvature, weights, ids_ref, theta_ref, phi_ref, table_ref,
    psi_ref, modes_ref,
    F, W, YS, YR, ZS, ZR, PT, RED, MINE,
    load_sem, xs_sem, xr_sem, ys_sem, yr_sem, zs_sem, zr_sem, ps_sem, pr_sem,
):
    cx, cy, cz = psi_ref.shape[1:]
    here = {axis: lax.axis_index(axis) for axis in AXES}
    loads = [
        pltpu.make_async_copy(metric, F.at[pl.ds(0, 6), pl.ds(2, cx), pl.ds(LO, cy)], load_sem.at[0]),
        pltpu.make_async_copy(curvature, F.at[pl.ds(6, 6), pl.ds(2, cx), pl.ds(LO, cy)], load_sem.at[1]),
        pltpu.make_async_copy(weights, W, load_sem.at[2]),
    ]
    for copy in loads:
        copy.start()
    barrier = pltpu.get_barrier_semaphore()
    peers = 0
    for axis in AXES:
        for step in range(1, counts[axis]):
            pl.semaphore_signal(
                barrier, inc=1, device_id={axis: lax.rem(here[axis] + step, counts[axis])}, device_id_type=MESH
            )
            peers += 1
    pl.semaphore_wait(barrier, peers)

    def exchange(axis, make):
        me, count = here[axis], counts[axis]
        has = (me > 0, me < count - 1)
        target = ({axis: me - 1}, {axis: me + 1})
        return has, [make(side, target[side]) for side in range(2)]

    def x_copies(side, target):
        start, land = (0, cx + 2) if side == 0 else (cx - 2, 0)
        return [
            pltpu.make_async_remote_copy(
                src_ref=array.at[:, pl.ds(start, 2)],
                dst_ref=F.at[pl.ds(6 * which, 6), pl.ds(land, 2), pl.ds(LO, cy)],
                send_sem=xs_sem.at[side, which],
                recv_sem=xr_sem.at[1 - side, which],
                device_id=target,
                device_id_type=MESH,
            )
            for which, array in enumerate((metric, curvature))
        ]

    def packed_copies(send, recv, send_sem, recv_sem, whole):
        def make(side, target):
            return [
                pltpu.make_async_remote_copy(
                    src_ref=send if whole else send.at[side],
                    dst_ref=recv.at[1 - side],
                    send_sem=send_sem.at[side],
                    recv_sem=recv_sem.at[1 - side],
                    device_id=target,
                    device_id_type=MESH,
                )
            ]

        return make

    def start(has, copies):
        for side in range(2):
            @pl.when(has[side])
            def _():
                for copy in copies[side]:
                    copy.start()

    x_has, x_moves = exchange("gx", x_copies)
    start(x_has, x_moves)
    loads[0].wait()
    loads[1].wait()
    for side, row in ((0, LO), (1, LO + cy - 2)):
        for comp in range(12):
            group, place = divmod(comp, 4)
            YS[side, group, :, 2 * place : 2 * place + 2, :] = F[comp, 2 : 2 + cx, row : row + 2, :]
    y_has, y_moves = exchange("gy", packed_copies(YS, YR, ys_sem, yr_sem, False))
    start(y_has, y_moves)
    lane = lax.broadcasted_iota(jnp.int32, (1, 1, cz), 2)
    window = ((lane + 2) & (cz - 1)) >> 2
    half = cx // 2

    @pl.loop(0, half)
    def _(x):
        packed = jnp.zeros((cy, cz), jnp.float32)
        for high in range(2):
            for comp in range(12):
                spot = comp + high * 16
                moved = pltpu.roll(F[comp, 2 + x + high * half, LO : LO + cy, :], 4 * spot, 1) if spot else F[comp, 2 + x, LO : LO + cy, :]
                packed = jnp.where(window[0] == spot, moved, packed)
        ZS[x] = packed

    z_has, z_moves = exchange("gz", packed_copies(ZS, ZR, zs_sem, zr_sem, True))
    start(z_has, z_moves)

    y_re, y_im, sphere = harmonics(ids_ref[...], theta_ref, phi_ref, table_ref[...])

    for side in range(2):
        @pl.when(x_has[side])
        def _(side=side):
            for copy in x_moves[1 - side]:
                copy.wait_recv()

        @pl.when(jnp.logical_not(x_has[side]))
        def _(side=side):
            F[:, (0, cx + 2)[side] : (0, cx + 2)[side] + 2, LO : LO + cy, :] = jnp.zeros((12, 2, cy, cz), jnp.float32)

        @pl.when(y_has[side])
        def _(side=side):
            y_moves[1 - side][0].wait_recv()

        @pl.when(jnp.logical_not(y_has[side]))
        def _(side=side):
            YR[side] = jnp.zeros(YR.shape[1:], jnp.float32)

        row = (LO - 2, LO + cy)[side]
        for comp in range(12):
            group, place = divmod(comp, 4)
            F[comp, 2 : 2 + cx, row : row + 2, :] = YR[side, group, :, 2 * place : 2 * place + 2, :]

        @pl.when(z_has[side])
        def _(side=side):
            z_moves[1 - side][0].wait_recv()

        @pl.when(jnp.logical_not(z_has[side]))
        def _(side=side):
            ZR[side] = jnp.zeros(ZR.shape[1:], jnp.float32)

    def coordinate(axis, cells, index):
        return (here[axis] * cells + index).astype(jnp.float32) + (0.5 - counts[axis] * cells / 2.0)

    z = coordinate("gz", cz, lax.broadcasted_iota(jnp.int32, (8, cz), 1))

    @pl.loop(0, half)
    def _(x_low):
        for high in range(2):
            x_index = x_low + high * half
            x = coordinate("gx", cx, jnp.full((8, cz), x_index, jnp.int32))
            for part in range(cy // 8):
                rows = 8 * part
                y = coordinate("gy", cy, rows + lax.broadcasted_iota(jnp.int32, (8, cz), 0))

                def field(comp, dx, dy, rows=rows, x_index=x_index):
                    return F[comp, x_index + 2 + dx, LO + rows + dy : LO + rows + dy + 8, :]

                def halo(side, comp, rows=rows, high=high):
                    spot = 4 * (comp + 16 * high)
                    tile = ZR[side, x_low, rows : rows + 8, :]
                    return pltpu.roll(tile, (cz - spot) % cz, 1) if spot else tile

                real, imag = weyl_tile(
                    field, functools.partial(halo, 0), functools.partial(halo, 1), x, y, z
                )
                psi_ref[0, x_index, rows : rows + 8, :] = real.astype(jnp.bfloat16)
                psi_ref[1, x_index, rows : rows + 8, :] = imag.astype(jnp.bfloat16)
                both = jnp.concatenate([swap_blocks(real), swap_blocks(imag)], 0)
                PT[x_index, :, part * cz : (part + 1) * cz] = both.astype(jnp.bfloat16)

    loads[2].wait()
    width = BLK * BLK
    contract = (((1,), (1,)), ((), ()))
    acc = jnp.zeros((PT.shape[1], W.shape[0]), jnp.float32)
    for x_index in range(cx):
        acc = acc + lax.dot_general(
            PT[x_index], W[:, x_index * width : (x_index + 1) * width], contract, preferred_element_type=jnp.float32
        )
    blocks = cz // BLK
    row = lax.broadcasted_iota(jnp.int32, acc.shape, 0)
    slot = lax.broadcasted_iota(jnp.int32, acc.shape, 1)
    acc = jnp.where(row % blocks == slot // PB, acc, 0.0)
    v_re = jnp.sum(acc[:blocks], axis=0, keepdims=True)
    v_im = jnp.sum(acc[blocks:], axis=0, keepdims=True)
    row = lax.broadcasted_iota(jnp.int32, (8, W.shape[0]), 0)
    member = (row >> 1) == sphere
    even = (row & 1) == 0
    v_one = jnp.where(member, jnp.where(even, v_re, v_im), 0.0)
    v_two = jnp.where(member, jnp.where(even, v_im, -v_re), 0.0)
    highest = lax.Precision.HIGHEST
    local = lax.dot_general(v_one, y_re, contract, precision=highest, preferred_element_type=jnp.float32)
    local = local + lax.dot_general(v_two, y_im, contract, precision=highest, preferred_element_type=jnp.float32)
    local = local * (4.0 * math.pi / PTS)
    value = jnp.concatenate([local, jnp.zeros((8, 128 - ROWS), jnp.float32)], 1)

    base = 0
    sends = []
    for phase, axis in enumerate(AXES):
        me, count = here[axis], counts[axis]
        MINE[phase] = value
        moves = []
        for step in range(1, count):
            moves.append(
                pltpu.make_async_remote_copy(
                    src_ref=MINE.at[phase],
                    dst_ref=RED.at[base + me],
                    send_sem=ps_sem.at[base + step],
                    recv_sem=pr_sem.at[base + count - step],
                    device_id={axis: lax.rem(me + step, count)},
                    device_id_type=MESH,
                )
            )
        for move in moves:
            move.start()
        RED[base + me] = value
        for move in moves:
            move.wait_recv()
        value = RED[base]
        for rank in range(1, count):
            value = value + RED[base + rank]
        sends += moves
        base += count
    for s in range(SPHERES):
        modes_ref[s] = value[2 * s : 2 * s + 2, :MODES]
    for move in sends:
        move.wait_send()
    for has, moves in ((x_has, x_moves), (y_has, y_moves), (z_has, z_moves)):
        for side in range(2):
            @pl.when(has[side])
            def _(side=side, moves=moves):
                for copy in moves[side]:
                    copy.wait_send()


def shards(counts, metric_pert, curvature, interp_weights, point_ids, theta, phi):
    _, cx, cy, cz = metric_pert.shape
    blocks = interp_weights.shape[2]
    points = theta.shape[0]
    vmem = pl.BlockSpec(memory_space=pltpu.VMEM)
    anywhere = pl.BlockSpec(memory_space=pl.ANY)
    total = sum(counts.values())
    dma = pltpu.SemaphoreType.DMA
    f32 = jnp.float32
    return pl.pallas_call(
        functools.partial(kernel, counts),
        out_shape=(
            jax.ShapeDtypeStruct((2, cx, cy, cz), jnp.bfloat16),
            jax.ShapeDtypeStruct((SPHERES, 2, MODES), f32),
        ),
        in_specs=[anywhere] * 3 + [vmem] * 4,
        out_specs=(vmem, vmem),
        scratch_shapes=[
            pltpu.VMEM((12, cx + 4, LO + cy + 8, cz), f32),
            pltpu.VMEM((blocks * PB, BLK * BLK * BLK), jnp.bfloat16),
            pltpu.VMEM((2, 3, cx, 8, cz), f32),
            pltpu.VMEM((2, 3, cx, 8, cz), f32),
            pltpu.VMEM((cx // 2, cy, cz), f32),
            pltpu.VMEM((2, cx // 2, cy, cz), f32),
            pltpu.VMEM((cx, 2 * blocks, BLK * BLK), jnp.bfloat16),
            pltpu.VMEM((total, 8, 128), f32),
            pltpu.VMEM((3, 8, 128), f32),
            dma((3,)), dma((2, 2)), dma((2, 2)), dma((2,)), dma((2,)), dma((2,)), dma((2,)),
            dma((total,)), dma((total,)),
        ],
        compiler_params=pltpu.CompilerParams(
            collective_id=0, has_side_effects=True, vmem_limit_bytes=48 * 1024 * 1024
        ),
    )(
        metric_pert,
        curvature,
        interp_weights.reshape(blocks * PB, BLK * BLK * BLK),
        point_ids.reshape(blocks, PB),
        theta.reshape(points // 128, 128),
        phi.reshape(points // 128, 128),
        jnp.asarray(build_table()),
    )


def solution(mesh):
    in_specs = (
        P(None, "gx", "gy", "gz"),
        P(None, "gx", "gy", "gz"),
        P("gx", "gy", "gz", None, None),
        P("gx", "gy", "gz", None),
        P(),
        P(),
    )
    out_specs = (P(None, "gx", "gy", "gz"), P())
    counts = {axis: mesh.shape[axis] for axis in AXES}
    return jax.shard_map(
        functools.partial(shards, counts), mesh=mesh, in_specs=in_specs, out_specs=out_specs, check_vma=False
    )
```

```python
import functools
import math

import jax
import jax.numpy as jnp
import numpy as np
from jax import lax
from jax.experimental import pallas as pl
from jax.experimental.pallas import tpu as pltpu
from jax.sharding import PartitionSpec as P

BLK = 16
PB = 64
PTS = 2048
SPHERES = 3
LMAX = 8
MODES = (LMAX + 1) ** 2 - 4
ROWS = -(-MODES // 8) * 8
AXES = ("gx", "gy", "gz")
PAIRS = [[0, 1, 2], [1, 3, 4], [2, 4, 5]]
MESH = pl.DeviceIdType.MESH
LO = 8


def build_table():
    table = np.zeros((ROWS, ROWS))
    for degree in range(2, LMAX + 1):
        base = degree * degree - 4
        for order in range(-degree, degree + 1):
            lead = (-1.0) ** order * math.sqrt(
                math.factorial(degree + order)
                * math.factorial(degree - order)
                * (2 * degree + 1)
                / (4.0 * math.pi * math.factorial(degree - 2) * math.factorial(degree + 2))
            )
            for step in range(0, degree + 3):
                lower = step - 2 - order
                if 0 <= lower <= degree - 2:
                    table[base + order + degree, base + 2 * step - 2 - order] += (
                        lead
                        * math.comb(degree + 2, step)
                        * math.comb(degree - 2, lower)
                        * (-1.0) ** (degree - step + 2)
                    )
    return table.astype(np.float32)


def power(bits, base, count):
    result = None
    for bit in range(count):
        factor = jnp.where((bits >> bit) & 1 == 1, base, 1.0)
        result = factor if result is None else result * factor
        base = base * base
    return result


def harmonics(ids, theta_ref, phi_ref, table):
    blocks, slots = ids.shape
    copies = 128 // slots
    wide = jnp.concatenate([ids] * copies, 1)
    safe = jnp.minimum(wide, SPHERES * PTS - 1)
    row, lane = safe >> 7, safe & 127
    theta = jnp.zeros(wide.shape, jnp.float32)
    phi = jnp.zeros(wide.shape, jnp.float32)
    for index in range(theta_ref.shape[0]):
        here = row == index
        one = jnp.broadcast_to(theta_ref[index : index + 1, :], wide.shape)
        theta = jnp.where(here, jnp.take_along_axis(one, lane, axis=1), theta)
        one = jnp.broadcast_to(phi_ref[index : index + 1, :], wide.shape)
        phi = jnp.where(here, jnp.take_along_axis(one, lane, axis=1), phi)

    def flat(array):
        return jnp.concatenate([array[b : b + 1, :slots] for b in range(blocks)], 1)

    half = theta * 0.5
    cosine, sine = flat(jnp.cos(half)), flat(jnp.sin(half))
    re, im = flat(jnp.cos(phi)), flat(jnp.sin(phi))
    sphere = flat(wide // PTS)
    k = lax.broadcasted_iota(jnp.int32, (ROWS, 1), 0)
    degree = jnp.full((ROWS, 1), 2, jnp.int32)
    for below in range(2, LMAX + 1):
        degree = degree + (k >= (below + 1) ** 2 - 4).astype(jnp.int32)
    first = k - (degree * degree - 4)
    order = first - degree
    mono = power(first, cosine, 5) * power(2 * degree - first, sine, 5)
    amplitude = jnp.dot(table, mono, precision=lax.Precision.HIGHEST, preferred_element_type=jnp.float32)
    size = jnp.abs(order)
    total_re = jnp.ones((ROWS, blocks * slots), jnp.float32)
    total_im = jnp.zeros((ROWS, blocks * slots), jnp.float32)
    for bit in range(4):
        on = (size >> bit) & 1 == 1
        f_re, f_im = jnp.where(on, re, 1.0), jnp.where(on, im, 0.0)
        total_re, total_im = total_re * f_re - total_im * f_im, total_re * f_im + total_im * f_re
        re, im = re * re - im * im, 2.0 * re * im
    total_im = jnp.where(order < 0, -total_im, total_im)
    return amplitude * total_re, amplitude * total_im, sphere


def curls(deriv):
    def minus(one, two):
        if two is None:
            return one
        return -two if one is None else one - two

    def plus(one, two):
        if one is None or two is None:
            return two if one is None else one
        return one + two

    def curl(row, col):
        one, two = (row + 1) % 3, (row + 2) % 3
        return minus(deriv(one, PAIRS[two][col]), deriv(two, PAIRS[one][col]))

    magnetic = {}
    for row in range(3):
        magnetic[row, row] = curl(row, row)
        for col in range(row + 1, 3):
            both = plus(curl(row, col), curl(col, row))
            magnetic[row, col] = None if both is None else 0.5 * both
    return magnetic


def contract_frame(electric, magnetic, x, y, z):
    rho2 = x * x + y * y
    rho = jnp.sqrt(rho2)
    radius = jnp.sqrt(rho2 + z * z)
    inv_rho, inv_radius = 1.0 / rho, 1.0 / radius
    cos_phi, sin_phi = x * inv_rho, y * inv_rho
    cos_theta, sin_theta = z * inv_radius, rho * inv_radius
    t = [cos_theta * cos_phi, cos_theta * sin_phi, -sin_theta]
    p = [-sin_phi, cos_phi, None]
    real, imag = 0.0, 0.0
    for row in range(3):
        for col in range(row, 3):
            weight = 0.5 if row == col else 1.0
            plus = t[row] * t[col]
            if col < 2:
                plus = plus - p[row] * p[col]
            plus = plus * weight
            cross = None
            if row < 2:
                cross = p[row] * t[col]
                if col < 2:
                    cross = cross + t[row] * p[col]
                cross = cross * weight
            e, b = electric[row, col], magnetic[row, col]
            real = real + e * plus
            if b is not None:
                imag = imag - b * plus
            if cross is not None:
                imag = imag - e * cross
                if b is not None:
                    real = real - b * cross
    return real, imag


def face_tile(axis, sign, near, far, x, y, z):
    def combine(comp, one, two):
        beside = near(comp)
        value = far(comp) * (-two)
        return value if beside is None else value + beside * one

    electric = {}
    for row in range(3):
        for col in range(row, 3):
            electric[row, col] = combine(PAIRS[row][col], 16.0 / 12.0, 1.0 / 12.0) * -0.5
    deriv = functools.lru_cache(None)(
        lambda along, comp: combine(6 + comp, 8.0 / 12.0, 1.0 / 12.0) * sign if along == axis else None
    )
    return contract_frame(electric, curls(deriv), x, y, z)


def weyl_tile(field, x, y, z):
    lane = lax.broadcasted_iota(jnp.int32, z.shape, 1)
    last = z.shape[1]

    def along(comp, axis, offset):
        if axis == 0:
            return field(comp, offset, 0)
        if axis == 1:
            return field(comp, 0, offset)
        outside = lane < offset if offset > 0 else lane >= last + offset
        return pltpu.roll(jnp.where(outside, 0.0, field(comp, 0, 0)), (-offset) % last, 1)

    def first(comp, axis):
        near = along(comp, axis, 1) - along(comp, axis, -1)
        far = along(comp, axis, 2) - along(comp, axis, -2)
        return near * (8.0 / 12.0) - far * (1.0 / 12.0)

    k = [field(6 + comp, 0, 0) for comp in range(6)]
    trace = k[0] + k[3] + k[5]
    electric = {}
    for row in range(3):
        for col in range(row, 3):
            comp = PAIRS[row][col]
            near, far = 0.0, 0.0
            for axis in range(3):
                near = near + (along(comp, axis, 1) + along(comp, axis, -1))
                far = far + (along(comp, axis, 2) + along(comp, axis, -2))
            laplace = near * (16.0 / 12.0) - far * (1.0 / 12.0) - field(comp, 0, 0) * 7.5
            square = sum(k[PAIRS[row][l]] * k[PAIRS[l][col]] for l in range(3))
            electric[row, col] = trace * k[comp] - square - 0.5 * laplace
    deriv = functools.lru_cache(None)(lambda axis, comp: first(6 + comp, axis))
    return contract_frame(electric, curls(deriv), x, y, z)


def swap_blocks(tile):
    count = tile.shape[0]
    width = tile.shape[1] // count
    rolled = pltpu.roll(tile, 0, 1, stride=width, stride_axis=0)
    row = lax.broadcasted_iota(jnp.int32, tile.shape, 0)
    block = lax.broadcasted_iota(jnp.int32, tile.shape, 1) // width
    mixed = jnp.take_along_axis(rolled, (block - row + count) % count, axis=0)
    out = mixed
    for bit in range(3):
        shift = (1 << bit) * width
        out = jnp.where((row >> bit) & 1 == 1, pltpu.roll(out, tile.shape[1] - shift, 1), out)
    return out


def kernel(
    counts, metric, curvature, weights, ids_hbm, theta_hbm, phi_hbm, table_hbm,
    psi_ref, modes_ref,
    F, W, ids_ref, theta_ref, phi_ref, table_ref, PS, XS, XR, YS, YR, ZS, ZR, PT, RED, MINE,
    load_sem, xs_sem, xr_sem, ys_sem, yr_sem, zs_sem, zr_sem, ps_sem, pr_sem,
):
    cx, cy, cz = psi_ref.shape[1:]
    here = {axis: lax.axis_index(axis) for axis in AXES}
    loads = [
        pltpu.make_async_copy(source, target, load_sem.at[place])
        for place, (source, target) in enumerate((
            (metric, F.at[pl.ds(0, 6), pl.ds(2, cx), pl.ds(LO, cy)]),
            (curvature, F.at[pl.ds(6, 6), pl.ds(2, cx), pl.ds(LO, cy)]),
            (ids_hbm, ids_ref),
            (theta_hbm, theta_ref),
            (phi_hbm, phi_ref),
            (table_hbm, table_ref),
            (weights, W),
        ))
    ]
    for copy in loads:
        copy.start()
    plane = counts["gx"] * counts["gy"]
    rank = here["gx"] * counts["gy"] + here["gy"]

    def in_plane(step):
        other = lax.rem(rank + step, plane)
        return {"gx": other // counts["gy"], "gy": lax.rem(other, counts["gy"])}

    def in_column(step):
        return {"gz": lax.rem(here["gz"] + step, counts["gz"])}

    groups = ((rank, plane, in_plane), (here["gz"], counts["gz"], in_column))
    barrier = pltpu.get_barrier_semaphore()
    for _, count, peer in groups:
        for step in range(1, count):
            pl.semaphore_signal(barrier, inc=1, device_id=peer(step), device_id_type=MESH)

    for edge in (0, cx + 2):
        F[:, edge : edge + 2, LO : LO + cy, :] = jnp.zeros((12, 2, cy, cz), jnp.float32)
    for edge in (LO - 8, LO + cy):
        F[:, 2 : 2 + cx, edge : edge + 8, :] = jnp.zeros((12, cx, 8, cz), jnp.float32)

    def coordinate(axis, cells, index):
        return (here[axis] * cells + index).astype(jnp.float32) + (0.5 - counts[axis] * cells / 2.0)

    loads[0].wait()
    loads[1].wait()
    tile = (8, cz)
    sub = lax.broadcasted_iota(jnp.int32, tile, 0)
    lane = lax.broadcasted_iota(jnp.int32, tile, 1)
    z = coordinate("gz", cz, lane)

    def layers(cells):
        return (
            (0, 0, -2, None, 0), (0, 1, -1, 0, 1),
            (1, 0, cells, cells - 1, cells - 2), (1, 1, cells + 1, None, cells - 1),
        )

    for side, layer, cell, near, far in layers(cx):
        for part in range(cy // 8):
            rows = slice(LO + 8 * part, LO + 8 * part + 8)
            load = lambda at, rows=rows: lambda comp: None if at is None else F[comp, 2 + at, rows, :]
            real, imag = face_tile(
                0, 1.0 - 2.0 * side, load(near), load(far),
                coordinate("gx", cx, jnp.full(tile, cell, jnp.int32)), coordinate("gy", cy, sub + 8 * part), z,
            )
            XS[side, 0, layer, 8 * part : 8 * part + 8, :] = real
            XS[side, 1, layer, 8 * part : 8 * part + 8, :] = imag
    for side, layer, cell, near, far in layers(cy):
        for part in range(cx // 8):
            rows = slice(2 + 8 * part, 2 + 8 * part + 8)
            load = lambda at, rows=rows: lambda comp: None if at is None else F[comp, rows, LO + at, :]
            real, imag = face_tile(
                1, 1.0 - 2.0 * side, load(near), load(far),
                coordinate("gx", cx, sub + 8 * part), coordinate("gy", cy, jnp.full(tile, cell, jnp.int32)), z,
            )
            YS[side, 0, layer, 8 * part : 8 * part + 8, :] = real
            YS[side, 1, layer, 8 * part : 8 * part + 8, :] = imag

    spot_of = ((lane + 2) & (cz - 1)) >> 2
    place = (lane + 2) & 3

    @functools.lru_cache(None)
    def z_edges(comp):
        packed = None
        for part in range(cy // 8):
            for x in range(cx):
                spot = part * cx + x
                moved = F[comp, 2 + x, LO + 8 * part : LO + 8 * part + 8, :]
                if spot:
                    moved = jnp.where(spot_of == spot, pltpu.roll(moved, 4 * spot, 1), packed)
                packed = moved
        return packed

    def z_near(comp):
        edges = z_edges(comp)
        return jnp.where(place == 3, pltpu.roll(edges, 1, 1), jnp.where(place == 0, pltpu.roll(edges, cz - 1, 1), 0.0))

    real, imag = face_tile(
        2, jnp.where(place >= 2, 1.0, -1.0), functools.lru_cache(None)(z_near), z_edges,
        coordinate("gx", cx, spot_of % cx), coordinate("gy", cy, (spot_of // cx) * 8 + sub),
        coordinate("gz", cz, jnp.where(place >= 2, place - 4, cz + place)),
    )
    ZS[0] = real
    ZS[1] = imag

    pl.semaphore_wait(barrier, sum(count - 1 for _, count, _ in groups))

    moves = []
    for axis, send, recv, send_sem, recv_sem in (
        ("gx", XS, XR, xs_sem, xr_sem), ("gy", YS, YR, ys_sem, yr_sem), ("gz", ZS, ZR, zs_sem, zr_sem)
    ):
        for side, has, target in ((0, here[axis] > 0, -1), (1, here[axis] < counts[axis] - 1, 1)):
            move = pltpu.make_async_remote_copy(
                src_ref=send if axis == "gz" else send.at[side],
                dst_ref=recv.at[1 - side],
                send_sem=send_sem.at[side],
                recv_sem=recv_sem.at[1 - side],
                device_id={axis: here[axis] + target},
                device_id_type=MESH,
            )
            arrival = pltpu.make_async_remote_copy(
                src_ref=send if axis == "gz" else send.at[side],
                dst_ref=recv.at[side],
                send_sem=send_sem.at[side],
                recv_sem=recv_sem.at[side],
                device_id={axis: here[axis] + target},
                device_id_type=MESH,
            )
            moves.append((has, move, arrival, recv, side))

            @pl.when(has)
            def _(move=move):
                move.start()

    @pl.loop(0, cx)
    def _(x_index):
        x = coordinate("gx", cx, jnp.full(tile, x_index, jnp.int32))
        for part in range(cy // 8):
            rows = 8 * part
            y = coordinate("gy", cy, rows + sub)

            def field(comp, dx, dy, rows=rows):
                return F[comp, x_index + 2 + dx, LO + rows + dy : LO + rows + dy + 8, :]

            real, imag = weyl_tile(field, x, y, z)
            PS[0, x_index, rows : rows + 8, :] = real
            PS[1, x_index, rows : rows + 8, :] = imag

    for copy in loads[2:6]:
        copy.wait()
    y_re, y_im, sphere = harmonics(ids_ref[...], theta_ref, phi_ref, table_ref[...])

    for has, move, arrival, recv, side in moves:
        @pl.when(has)
        def _(arrival=arrival):
            arrival.wait_recv()

        @pl.when(jnp.logical_not(has))
        def _(recv=recv, side=side):
            recv[side] = jnp.zeros(recv.shape[1:], jnp.float32)

    for side in range(2):
        for layer in range(2):
            x_at, y_at = layer + side * (cx - 2), layer + side * (cy - 2)
            for c in range(2):
                PS[c, x_at] = PS[c, x_at] + XR[side, c, layer]
                PS[c, :, y_at, :] = PS[c, :, y_at, :] + YR[side, c, layer]
    for c in range(2):
        ZS2 = jnp.where(place < 2, pltpu.roll(ZR[1, c], cz - 2, 1), pltpu.roll(ZR[0, c], 2, 1))
        MINE[c] = ZS2
    rim = (lane < 2) | (lane >= cz - 2)

    @pl.loop(0, cx)
    def _(x_index):
        for part in range(cy // 8):
            rows = 8 * part
            both = []
            for c in range(2):
                extra = pltpu.roll(MINE[c], lax.rem(2 * cz - 4 * (part * cx + x_index), cz), 1)
                value = PS[c, x_index, rows : rows + 8, :] + jnp.where(rim, extra, 0.0)
                psi_ref[c, x_index, rows : rows + 8, :] = value.astype(jnp.bfloat16)
                both.append(swap_blocks(value))
            PT[x_index, :, part * cz : (part + 1) * cz] = jnp.concatenate(both, 0).astype(jnp.bfloat16)

    loads[6].wait()
    width = BLK * BLK
    contract = (((1,), (1,)), ((), ()))
    acc = jnp.zeros((PT.shape[1], W.shape[0]), jnp.float32)
    for x_index in range(cx):
        acc = acc + lax.dot_general(
            PT[x_index], W[:, x_index * width : (x_index + 1) * width], contract, preferred_element_type=jnp.float32
        )
    blocks = cz // BLK
    row = lax.broadcasted_iota(jnp.int32, acc.shape, 0)
    slot = lax.broadcasted_iota(jnp.int32, acc.shape, 1)
    acc = jnp.where(row % blocks == slot // PB, acc, 0.0)
    v_re = jnp.sum(acc[:blocks], axis=0, keepdims=True)
    v_im = jnp.sum(acc[blocks:], axis=0, keepdims=True)
    row = lax.broadcasted_iota(jnp.int32, (8, W.shape[0]), 0)
    member = (row >> 1) == sphere
    even = (row & 1) == 0
    v_one = jnp.where(member, jnp.where(even, v_re, v_im), 0.0)
    v_two = jnp.where(member, jnp.where(even, v_im, -v_re), 0.0)
    highest = lax.Precision.HIGHEST
    local = lax.dot_general(v_one, y_re, contract, precision=highest, preferred_element_type=jnp.float32)
    local = local + lax.dot_general(v_two, y_im, contract, precision=highest, preferred_element_type=jnp.float32)
    local = local * (4.0 * math.pi / PTS)
    value = jnp.concatenate([local, jnp.zeros((8, 128 - ROWS), jnp.float32)], 1)

    base = 0
    sends = []
    for phase, (me, count, peer) in enumerate(groups):
        MINE[2 + phase] = value
        copies = [
            pltpu.make_async_remote_copy(
                src_ref=MINE.at[2 + phase],
                dst_ref=RED.at[base + me],
                send_sem=ps_sem.at[base + step],
                recv_sem=pr_sem.at[base + count - step],
                device_id=peer(step),
                device_id_type=MESH,
            )
            for step in range(1, count)
        ]
        for copy in copies:
            copy.start()
        RED[base + me] = value
        for copy in copies:
            copy.wait_recv()
        value = RED[base]
        for other in range(1, count):
            value = value + RED[base + other]
        sends += copies
        base += count
    for s in range(SPHERES):
        modes_ref[s] = value[2 * s : 2 * s + 2, :MODES]
    for copy in sends:
        copy.wait_send()
    for has, move, _, _, _ in moves:
        @pl.when(has)
        def _(move=move):
            move.wait_send()


def shards(counts, metric_pert, curvature, interp_weights, point_ids, theta, phi):
    _, cx, cy, cz = metric_pert.shape
    blocks = interp_weights.shape[2]
    points = theta.shape[0]
    vmem = pl.BlockSpec(memory_space=pltpu.VMEM)
    anywhere = pl.BlockSpec(memory_space=pl.ANY)
    total = counts["gx"] * counts["gy"] + counts["gz"]
    dma = pltpu.SemaphoreType.DMA
    f32 = jnp.float32
    return pl.pallas_call(
        functools.partial(kernel, counts),
        out_shape=(
            jax.ShapeDtypeStruct((2, cx, cy, cz), jnp.bfloat16),
            jax.ShapeDtypeStruct((SPHERES, 2, MODES), f32),
        ),
        in_specs=[anywhere] * 7,
        out_specs=(vmem, vmem),
        scratch_shapes=[
            pltpu.VMEM((12, cx + 4, LO + cy + 8, cz), f32),
            pltpu.VMEM((blocks * PB, BLK * BLK * BLK), jnp.bfloat16),
            pltpu.VMEM((blocks, PB), jnp.int32),
            pltpu.VMEM((points // 128, 128), f32),
            pltpu.VMEM((points // 128, 128), f32),
            pltpu.VMEM((ROWS, ROWS), f32),
            pltpu.VMEM((2, cx, cy, cz), f32),
            pltpu.VMEM((2, 2, 2, cy, cz), f32),
            pltpu.VMEM((2, 2, 2, cy, cz), f32),
            pltpu.VMEM((2, 2, 2, cx, cz), f32),
            pltpu.VMEM((2, 2, 2, cx, cz), f32),
            pltpu.VMEM((2, 8, cz), f32),
            pltpu.VMEM((2, 2, 8, cz), f32),
            pltpu.VMEM((cx, 2 * blocks, BLK * BLK), jnp.bfloat16),
            pltpu.VMEM((total, 8, 128), f32),
            pltpu.VMEM((4, 8, 128), f32),
            dma((7,)), dma((2,)), dma((2,)), dma((2,)), dma((2,)), dma((2,)), dma((2,)),
            dma((total,)), dma((total,)),
        ],
        compiler_params=pltpu.CompilerParams(
            collective_id=0, has_side_effects=True, vmem_limit_bytes=67043328 - 160 * 1024
        ),
    )(
        metric_pert,
        curvature,
        interp_weights.reshape(blocks * PB, BLK * BLK * BLK),
        point_ids.reshape(blocks, PB),
        theta.reshape(points // 128, 128),
        phi.reshape(points // 128, 128),
        jnp.asarray(build_table()),
    )


def solution(mesh):
    in_specs = (
        P(None, "gx", "gy", "gz"),
        P(None, "gx", "gy", "gz"),
        P("gx", "gy", "gz", None, None),
        P("gx", "gy", "gz", None),
        P(),
        P(),
    )
    out_specs = (P(None, "gx", "gy", "gz"), P())
    counts = {axis: mesh.shape[axis] for axis in AXES}
    return jax.shard_map(
        functools.partial(shards, counts), mesh=mesh, in_specs=in_specs, out_specs=out_specs, check_vma=False
    )
```

```python
import functools
import math

import jax
import jax.numpy as jnp
import numpy as np
from jax import lax
from jax.experimental import pallas as pl
from jax.experimental.pallas import tpu as pltpu
from jax.sharding import PartitionSpec as P

BLK = 16
PB = 64
PTS = 2048
SPHERES = 3
LMAX = 8
MODES = (LMAX + 1) ** 2 - 4
ROWS = -(-MODES // 8) * 8
AXES = ("gx", "gy", "gz")
PAIRS = [[0, 1, 2], [1, 3, 4], [2, 4, 5]]
MESH = pl.DeviceIdType.MESH
LO = 8


def build_table():
    table = np.zeros((ROWS, ROWS))
    for degree in range(2, LMAX + 1):
        base = degree * degree - 4
        for order in range(-degree, degree + 1):
            lead = (-1.0) ** order * math.sqrt(
                math.factorial(degree + order)
                * math.factorial(degree - order)
                * (2 * degree + 1)
                / (4.0 * math.pi * math.factorial(degree - 2) * math.factorial(degree + 2))
            )
            for step in range(0, degree + 3):
                lower = step - 2 - order
                if 0 <= lower <= degree - 2:
                    table[base + order + degree, base + 2 * step - 2 - order] += (
                        lead
                        * math.comb(degree + 2, step)
                        * math.comb(degree - 2, lower)
                        * (-1.0) ** (degree - step + 2)
                    )
    return table.astype(np.float32)


def power(bits, base, count):
    result = None
    for bit in range(count):
        factor = jnp.where((bits >> bit) & 1 == 1, base, 1.0)
        result = factor if result is None else result * factor
        base = base * base
    return result


def harmonics(ids, theta_ref, phi_ref, table):
    blocks, slots = ids.shape
    copies = 128 // slots
    wide = jnp.concatenate([ids] * copies, 1)
    safe = jnp.minimum(wide, SPHERES * PTS - 1)
    row, lane = safe >> 7, safe & 127
    theta = jnp.zeros(wide.shape, jnp.float32)
    phi = jnp.zeros(wide.shape, jnp.float32)
    for index in range(theta_ref.shape[0]):
        here = row == index
        one = jnp.broadcast_to(theta_ref[index : index + 1, :], wide.shape)
        theta = jnp.where(here, jnp.take_along_axis(one, lane, axis=1), theta)
        one = jnp.broadcast_to(phi_ref[index : index + 1, :], wide.shape)
        phi = jnp.where(here, jnp.take_along_axis(one, lane, axis=1), phi)

    def flat(array):
        return jnp.concatenate([array[b : b + 1, :slots] for b in range(blocks)], 1)

    half = theta * 0.5
    cosine, sine = flat(jnp.cos(half)), flat(jnp.sin(half))
    re, im = flat(jnp.cos(phi)), flat(jnp.sin(phi))
    sphere = flat(wide // PTS)
    k = lax.broadcasted_iota(jnp.int32, (ROWS, 1), 0)
    degree = jnp.full((ROWS, 1), 2, jnp.int32)
    for below in range(2, LMAX + 1):
        degree = degree + (k >= (below + 1) ** 2 - 4).astype(jnp.int32)
    first = k - (degree * degree - 4)
    order = first - degree
    mono = power(first, cosine, 5) * power(2 * degree - first, sine, 5)
    amplitude = jnp.dot(table, mono, precision=lax.Precision.HIGHEST, preferred_element_type=jnp.float32)
    size = jnp.abs(order)
    total_re = jnp.ones((ROWS, blocks * slots), jnp.float32)
    total_im = jnp.zeros((ROWS, blocks * slots), jnp.float32)
    for bit in range(4):
        on = (size >> bit) & 1 == 1
        f_re, f_im = jnp.where(on, re, 1.0), jnp.where(on, im, 0.0)
        total_re, total_im = total_re * f_re - total_im * f_im, total_re * f_im + total_im * f_re
        re, im = re * re - im * im, 2.0 * re * im
    total_im = jnp.where(order < 0, -total_im, total_im)
    return amplitude * total_re, amplitude * total_im, sphere


def curls(deriv):
    def minus(one, two):
        if two is None:
            return one
        return -two if one is None else one - two

    def plus(one, two):
        if one is None or two is None:
            return two if one is None else one
        return one + two

    def curl(row, col):
        one, two = (row + 1) % 3, (row + 2) % 3
        return minus(deriv(one, PAIRS[two][col]), deriv(two, PAIRS[one][col]))

    magnetic = {}
    for row in range(3):
        magnetic[row, row] = curl(row, row)
        for col in range(row + 1, 3):
            both = plus(curl(row, col), curl(col, row))
            magnetic[row, col] = None if both is None else 0.5 * both
    return magnetic


def contract_frame(electric, magnetic, x, y, z):
    rho2 = x * x + y * y
    rho = jnp.sqrt(rho2)
    radius = jnp.sqrt(rho2 + z * z)
    inv_rho, inv_radius = 1.0 / rho, 1.0 / radius
    cos_phi, sin_phi = x * inv_rho, y * inv_rho
    cos_theta, sin_theta = z * inv_radius, rho * inv_radius
    t = [cos_theta * cos_phi, cos_theta * sin_phi, -sin_theta]
    p = [-sin_phi, cos_phi, None]
    real, imag = 0.0, 0.0
    for row in range(3):
        for col in range(row, 3):
            weight = 0.5 if row == col else 1.0
            plus = t[row] * t[col]
            if col < 2:
                plus = plus - p[row] * p[col]
            plus = plus * weight
            cross = None
            if row < 2:
                cross = p[row] * t[col]
                if col < 2:
                    cross = cross + t[row] * p[col]
                cross = cross * weight
            e, b = electric[row, col], magnetic[row, col]
            real = real + e * plus
            if b is not None:
                imag = imag - b * plus
            if cross is not None:
                imag = imag - e * cross
                if b is not None:
                    real = real - b * cross
    return real, imag


def face_tile(axis, sign, near, far, x, y, z):
    def combine(comp, one, two):
        beside = near(comp)
        value = far(comp) * (-two)
        return value if beside is None else value + beside * one

    electric = {}
    for row in range(3):
        for col in range(row, 3):
            electric[row, col] = combine(PAIRS[row][col], 16.0 / 12.0, 1.0 / 12.0) * -0.5
    deriv = functools.lru_cache(None)(
        lambda along, comp: combine(6 + comp, 8.0 / 12.0, 1.0 / 12.0) * sign if along == axis else None
    )
    return contract_frame(electric, curls(deriv), x, y, z)


def weyl_tile(field, x, y, z):
    lane = lax.broadcasted_iota(jnp.int32, z.shape, 1)
    last = z.shape[1]

    def along(comp, axis, offset):
        if axis == 0:
            return field(comp, offset, 0)
        if axis == 1:
            return field(comp, 0, offset)
        outside = lane < offset if offset > 0 else lane >= last + offset
        return pltpu.roll(jnp.where(outside, 0.0, field(comp, 0, 0)), (-offset) % last, 1)

    def first(comp, axis):
        near = along(comp, axis, 1) - along(comp, axis, -1)
        far = along(comp, axis, 2) - along(comp, axis, -2)
        return near * (8.0 / 12.0) - far * (1.0 / 12.0)

    k = [field(6 + comp, 0, 0) for comp in range(6)]
    trace = k[0] + k[3] + k[5]
    electric = {}
    for row in range(3):
        for col in range(row, 3):
            comp = PAIRS[row][col]
            near, far = 0.0, 0.0
            for axis in range(3):
                near = near + (along(comp, axis, 1) + along(comp, axis, -1))
                far = far + (along(comp, axis, 2) + along(comp, axis, -2))
            laplace = near * (16.0 / 12.0) - far * (1.0 / 12.0) - field(comp, 0, 0) * 7.5
            square = sum(k[PAIRS[row][l]] * k[PAIRS[l][col]] for l in range(3))
            electric[row, col] = trace * k[comp] - square - 0.5 * laplace
    deriv = functools.lru_cache(None)(lambda axis, comp: first(6 + comp, axis))
    return contract_frame(electric, curls(deriv), x, y, z)


def swap_blocks(tile):
    count = tile.shape[0]
    width = tile.shape[1] // count
    rolled = pltpu.roll(tile, 0, 1, stride=width, stride_axis=0)
    row = lax.broadcasted_iota(jnp.int32, tile.shape, 0)
    block = lax.broadcasted_iota(jnp.int32, tile.shape, 1) // width
    mixed = jnp.take_along_axis(rolled, (block - row + count) % count, axis=0)
    out = mixed
    for bit in range(3):
        shift = (1 << bit) * width
        out = jnp.where((row >> bit) & 1 == 1, pltpu.roll(out, tile.shape[1] - shift, 1), out)
    return out


def kernel(
    counts, metric, curvature, weights, ids_hbm, theta_hbm, phi_hbm, table_hbm,
    psi_ref, modes_ref,
    F, W, ids_ref, theta_ref, phi_ref, table_ref, PS, XS, XR, YS, YR, ZS, ZR, RED, MINE,
    load_sem, xs_sem, xr_sem, ys_sem, yr_sem, zs_sem, zr_sem, ps_sem, pr_sem,
):
    cx, cy, cz = psi_ref.shape[1:]
    here = {axis: lax.axis_index(axis) for axis in AXES}
    loads = [
        pltpu.make_async_copy(source, target, load_sem.at[place])
        for place, (source, target) in enumerate((
            (metric, F.at[pl.ds(0, 6), pl.ds(2, cx), pl.ds(LO, cy)]),
            (curvature, F.at[pl.ds(6, 6), pl.ds(2, cx), pl.ds(LO, cy)]),
            (ids_hbm, ids_ref),
            (theta_hbm, theta_ref),
            (phi_hbm, phi_ref),
            (table_hbm, table_ref),
            (weights, W),
        ))
    ]
    for copy in loads:
        copy.start()
    plane = counts["gx"] * counts["gy"]
    rank = here["gx"] * counts["gy"] + here["gy"]

    def in_plane(step):
        other = lax.rem(rank + step, plane)
        return {"gx": other // counts["gy"], "gy": lax.rem(other, counts["gy"])}

    def in_column(step):
        return {"gz": lax.rem(here["gz"] + step, counts["gz"])}

    groups = ((rank, plane, in_plane), (here["gz"], counts["gz"], in_column))
    barrier = pltpu.get_barrier_semaphore()
    for _, count, peer in groups:
        for step in range(1, count):
            pl.semaphore_signal(barrier, inc=1, device_id=peer(step), device_id_type=MESH)

    for edge in (0, cx + 2):
        F[:, edge : edge + 2, LO : LO + cy, :] = jnp.zeros((12, 2, cy, cz), jnp.float32)
    for edge in (LO - 8, LO + cy):
        F[:, 2 : 2 + cx, edge : edge + 8, :] = jnp.zeros((12, cx, 8, cz), jnp.float32)

    def coordinate(axis, cells, index):
        return (here[axis] * cells + index).astype(jnp.float32) + (0.5 - counts[axis] * cells / 2.0)

    loads[0].wait()
    loads[1].wait()
    tile = (8, cz)
    sub = lax.broadcasted_iota(jnp.int32, tile, 0)
    lane = lax.broadcasted_iota(jnp.int32, tile, 1)
    z = coordinate("gz", cz, lane)

    def layers(cells):
        return (
            (0, 0, -2, None, 0), (0, 1, -1, 0, 1),
            (1, 0, cells, cells - 1, cells - 2), (1, 1, cells + 1, None, cells - 1),
        )

    for side, layer, cell, near, far in layers(cx):
        for part in range(cy // 8):
            rows = slice(LO + 8 * part, LO + 8 * part + 8)
            load = lambda at, rows=rows: lambda comp: None if at is None else F[comp, 2 + at, rows, :]
            real, imag = face_tile(
                0, 1.0 - 2.0 * side, load(near), load(far),
                coordinate("gx", cx, jnp.full(tile, cell, jnp.int32)), coordinate("gy", cy, sub + 8 * part), z,
            )
            XS[side, 0, layer, 8 * part : 8 * part + 8, :] = real
            XS[side, 1, layer, 8 * part : 8 * part + 8, :] = imag
    for side, layer, cell, near, far in layers(cy):
        for part in range(cx // 8):
            rows = slice(2 + 8 * part, 2 + 8 * part + 8)
            load = lambda at, rows=rows: lambda comp: None if at is None else F[comp, rows, LO + at, :]
            real, imag = face_tile(
                1, 1.0 - 2.0 * side, load(near), load(far),
                coordinate("gx", cx, sub + 8 * part), coordinate("gy", cy, jnp.full(tile, cell, jnp.int32)), z,
            )
            YS[side, 0, layer, 8 * part : 8 * part + 8, :] = real
            YS[side, 1, layer, 8 * part : 8 * part + 8, :] = imag

    spot_of = ((lane + 2) & (cz - 1)) >> 2
    place = (lane + 2) & 3

    @functools.lru_cache(None)
    def z_edges(comp):
        packed = None
        for part in range(cy // 8):
            for x in range(cx):
                spot = part * cx + x
                moved = F[comp, 2 + x, LO + 8 * part : LO + 8 * part + 8, :]
                if spot:
                    moved = jnp.where(spot_of == spot, pltpu.roll(moved, 4 * spot, 1), packed)
                packed = moved
        return packed

    def z_near(comp):
        edges = z_edges(comp)
        return jnp.where(place == 3, pltpu.roll(edges, 1, 1), jnp.where(place == 0, pltpu.roll(edges, cz - 1, 1), 0.0))

    real, imag = face_tile(
        2, jnp.where(place >= 2, 1.0, -1.0), functools.lru_cache(None)(z_near), z_edges,
        coordinate("gx", cx, spot_of % cx), coordinate("gy", cy, (spot_of // cx) * 8 + sub),
        coordinate("gz", cz, jnp.where(place >= 2, place - 4, cz + place)),
    )
    ZS[0] = real
    ZS[1] = imag

    pl.semaphore_wait(barrier, sum(count - 1 for _, count, _ in groups))

    moves = []
    for axis, send, recv, send_sem, recv_sem in (
        ("gx", XS, XR, xs_sem, xr_sem), ("gy", YS, YR, ys_sem, yr_sem), ("gz", ZS, ZR, zs_sem, zr_sem)
    ):
        for side, has, target in ((0, here[axis] > 0, -1), (1, here[axis] < counts[axis] - 1, 1)):
            move = pltpu.make_async_remote_copy(
                src_ref=send if axis == "gz" else send.at[side],
                dst_ref=recv.at[1 - side],
                send_sem=send_sem.at[side],
                recv_sem=recv_sem.at[1 - side],
                device_id={axis: here[axis] + target},
                device_id_type=MESH,
            )
            arrival = pltpu.make_async_remote_copy(
                src_ref=send if axis == "gz" else send.at[side],
                dst_ref=recv.at[side],
                send_sem=send_sem.at[side],
                recv_sem=recv_sem.at[side],
                device_id={axis: here[axis] + target},
                device_id_type=MESH,
            )
            moves.append((has, move, arrival, recv, side))

            @pl.when(has)
            def _(move=move):
                move.start()

    @pl.loop(0, cx)
    def _(x_index):
        x = coordinate("gx", cx, jnp.full(tile, x_index, jnp.int32))
        for part in range(cy // 8):
            rows = 8 * part
            y = coordinate("gy", cy, rows + sub)

            def field(comp, dx, dy, rows=rows):
                return F[comp, x_index + 2 + dx, LO + rows + dy : LO + rows + dy + 8, :]

            real, imag = weyl_tile(field, x, y, z)
            PS[0, x_index, rows : rows + 8, :] = real
            PS[1, x_index, rows : rows + 8, :] = imag

    for copy in loads[2:6]:
        copy.wait()
    y_re, y_im, sphere = harmonics(ids_ref[...], theta_ref, phi_ref, table_ref[...])

    for has, move, arrival, recv, side in moves:
        @pl.when(has)
        def _(arrival=arrival):
            arrival.wait_recv()

        @pl.when(jnp.logical_not(has))
        def _(recv=recv, side=side):
            recv[side] = jnp.zeros(recv.shape[1:], jnp.float32)

    for side in range(2):
        for layer in range(2):
            x_at, y_at = layer + side * (cx - 2), layer + side * (cy - 2)
            for c in range(2):
                PS[c, x_at] = PS[c, x_at] + XR[side, c, layer]
                PS[c, :, y_at, :] = PS[c, :, y_at, :] + YR[side, c, layer]
    z_extra = [
        jnp.where(place < 2, pltpu.roll(ZR[1, c], cz - 2, 1), pltpu.roll(ZR[0, c], 2, 1)) for c in range(2)
    ]
    rim = (lane < 2) | (lane >= cz - 2)
    loads[6].wait()
    width = BLK * BLK
    contract = (((1,), (1,)), ((), ()))
    acc = jnp.zeros((2 * cz // BLK, W.shape[0]), jnp.float32)
    for x_index in range(cx):
        pieces = []
        for part in range(cy // 8):
            rows = 8 * part
            both = []
            for c in range(2):
                spot = part * cx + x_index
                extra = pltpu.roll(z_extra[c], cz - 4 * spot, 1) if spot else z_extra[c]
                value = PS[c, x_index, rows : rows + 8, :] + jnp.where(rim, extra, 0.0)
                psi_ref[c, x_index, rows : rows + 8, :] = value.astype(jnp.bfloat16)
                both.append(swap_blocks(value))
            pieces.append(jnp.concatenate(both, 0).astype(jnp.bfloat16))
        acc = acc + lax.dot_general(
            jnp.concatenate(pieces, 1),
            W[:, x_index * width : (x_index + 1) * width],
            contract,
            preferred_element_type=jnp.float32,
        )
    blocks = cz // BLK
    row = lax.broadcasted_iota(jnp.int32, acc.shape, 0)
    slot = lax.broadcasted_iota(jnp.int32, acc.shape, 1)
    acc = jnp.where(row % blocks == slot // PB, acc, 0.0)
    v_re = jnp.sum(acc[:blocks], axis=0, keepdims=True)
    v_im = jnp.sum(acc[blocks:], axis=0, keepdims=True)
    row = lax.broadcasted_iota(jnp.int32, (8, W.shape[0]), 0)
    member = (row >> 1) == sphere
    even = (row & 1) == 0
    v_one = jnp.where(member, jnp.where(even, v_re, v_im), 0.0)
    v_two = jnp.where(member, jnp.where(even, v_im, -v_re), 0.0)
    highest = lax.Precision.HIGHEST
    local = lax.dot_general(v_one, y_re, contract, precision=highest, preferred_element_type=jnp.float32)
    local = local + lax.dot_general(v_two, y_im, contract, precision=highest, preferred_element_type=jnp.float32)
    local = local * (4.0 * math.pi / PTS)
    value = jnp.concatenate([local, jnp.zeros((8, 128 - ROWS), jnp.float32)], 1)

    base = 0
    sends = []
    for phase, (me, count, peer) in enumerate(groups):
        MINE[phase] = value
        copies = [
            pltpu.make_async_remote_copy(
                src_ref=MINE.at[phase],
                dst_ref=RED.at[base + me],
                send_sem=ps_sem.at[base + step],
                recv_sem=pr_sem.at[base + count - step],
                device_id=peer(step),
                device_id_type=MESH,
            )
            for step in range(1, count)
        ]
        for copy in copies:
            copy.start()
        RED[base + me] = value
        for copy in copies:
            copy.wait_recv()
        value = RED[base]
        for other in range(1, count):
            value = value + RED[base + other]
        sends += copies
        base += count
    for s in range(SPHERES):
        modes_ref[s] = value[2 * s : 2 * s + 2, :MODES]
    for copy in sends:
        copy.wait_send()
    for has, move, _, _, _ in moves:
        @pl.when(has)
        def _(move=move):
            move.wait_send()


def shards(counts, metric_pert, curvature, interp_weights, point_ids, theta, phi):
    _, cx, cy, cz = metric_pert.shape
    blocks = interp_weights.shape[2]
    points = theta.shape[0]
    vmem = pl.BlockSpec(memory_space=pltpu.VMEM)
    anywhere = pl.BlockSpec(memory_space=pl.ANY)
    total = counts["gx"] * counts["gy"] + counts["gz"]
    dma = pltpu.SemaphoreType.DMA
    f32 = jnp.float32
    return pl.pallas_call(
        functools.partial(kernel, counts),
        out_shape=(
            pltpu.VMEM((2, cx, cy, cz), jnp.bfloat16),
            pltpu.VMEM((SPHERES, 2, MODES), f32),
        ),
        in_specs=[anywhere] * 7,
        out_specs=(vmem, vmem),
        scratch_shapes=[
            pltpu.VMEM((12, cx + 4, LO + cy + 8, cz), f32),
            pltpu.VMEM((blocks * PB, BLK * BLK * BLK), jnp.bfloat16),
            pltpu.VMEM((blocks, PB), jnp.int32),
            pltpu.VMEM((points // 128, 128), f32),
            pltpu.VMEM((points // 128, 128), f32),
            pltpu.VMEM((ROWS, ROWS), f32),
            pltpu.VMEM((2, cx, cy, cz), f32),
            pltpu.VMEM((2, 2, 2, cy, cz), f32),
            pltpu.VMEM((2, 2, 2, cy, cz), f32),
            pltpu.VMEM((2, 2, 2, cx, cz), f32),
            pltpu.VMEM((2, 2, 2, cx, cz), f32),
            pltpu.VMEM((2, 8, cz), f32),
            pltpu.VMEM((2, 2, 8, cz), f32),
            pltpu.VMEM((total, 8, 128), f32),
            pltpu.VMEM((2, 8, 128), f32),
            dma((7,)), dma((2,)), dma((2,)), dma((2,)), dma((2,)), dma((2,)), dma((2,)),
            dma((total,)), dma((total,)),
        ],
        compiler_params=pltpu.CompilerParams(
            collective_id=0, has_side_effects=True, vmem_limit_bytes=67043328 - 160 * 1024
        ),
    )(
        metric_pert,
        curvature,
        interp_weights.reshape(blocks * PB, BLK * BLK * BLK),
        point_ids.reshape(blocks, PB),
        theta.reshape(points // 128, 128),
        phi.reshape(points // 128, 128),
        jnp.asarray(build_table()),
    )


def solution(mesh):
    in_specs = (
        P(None, "gx", "gy", "gz"),
        P(None, "gx", "gy", "gz"),
        P("gx", "gy", "gz", None, None),
        P("gx", "gy", "gz", None),
        P(),
        P(),
    )
    out_specs = (P(None, "gx", "gy", "gz"), P())
    counts = {axis: mesh.shape[axis] for axis in AXES}
    return jax.shard_map(
        functools.partial(shards, counts), mesh=mesh, in_specs=in_specs, out_specs=out_specs, check_vma=False
    )
```
